32 devices in a mesh: seq: 8 (over z, x), tensor: 4 (over y, core).
Axes of the slice: x: 2, y: 2, z: 4, core: 2. Of those that a mesh axis runs over, the one named last changes fastest.
Arguments:
- hidden_in: bfloat16 [3072, 4096], P('seq', 'tensor'), may hold values from -6 to 6
- norm_gain: float32 [4096], replicated, may hold values from 0.5 to 1.5
- w_x: bfloat16 [4096, 8192], P('seq', 'tensor'), may hold values from -0.09375 to 0.09375
- w_z: bfloat16 [4096, 8192], P('seq', 'tensor'), may hold values from -0.09375 to 0.09375
- w_bc: bfloat16 [4096, 8, 256], P('seq', 'tensor'), may hold values from -0.09375 to 0.09375
- w_dt: bfloat16 [4096, 64], P('seq', 'tensor'), may hold values from -0.09375 to 0.09375
- dt_bias: float32 [64], P('tensor'), may hold values from -6 to -2
- decay_rate: float32 [64], P('tensor'), may hold values from 0.00032552084 to 8
- conv_x: float32 [4, 8192], P(None, 'tensor'), may hold values from -3 to 3
- conv_bc: float32 [4, 8, 256], P(None, 'tensor'), may hold values from -3 to 3
- conv_bias_x: float32 [8192], P('tensor'), may hold values from -3 to 3
- conv_bias_bc: float32 [8, 256], P('tensor'), may hold values from -3 to 3
- skip_d: float32 [64], P('tensor'), may hold values from 0.5 to 8
- out_gain: float32 [8192], P('tensor'), may hold values from 0.5 to 1.5
- w_out: bfloat16 [8192, 4096], P('tensor'), may hold values from -0.0625 to 0.0625
Outputs:
- layer_out: bfloat16 [3072, 4096], P('seq', 'tensor')
The draws below stay inside these ranges and needn't reach their ends.
All inputs are finite; a program needn't handle non-finite values.
Results may differ from the reference program's by a relative error of at most 0.0095.
Values may be sent and summed in bfloat16 or wider, within the bound.
A program may use at most 128 MiB of HBM per device.

```python
import math
import jax
import jax.numpy as jnp
from jax import lax

D = 4096
H = 64
P_SIZE = 128
N = 128
G = 8
KCONV = 4
SPAN = 128
DI = 8192
TOKENS = 3072


def shard_levels(stream_key, extent, cuts, smallest, largest):
    loudness, own = 1.0, jax.random.fold_in(stream_key, 6)
    for position, shards_of in cuts:
        draws = jnp.exp(jax.random.uniform(jax.random.fold_in(own, position), (shards_of,), jnp.float32, smallest / len(cuts), largest / len(cuts)))
        loudness = loudness * jnp.repeat(draws, extent[position] // shards_of).reshape([-1 if axis == position else 1 for axis in range(len(extent))])
    return loudness


def centred(stream_key, shape, deviation, most, split=(), dtype=jnp.bfloat16):
    gain = shard_levels(stream_key, shape, split, -0.22, 0.18) if split else 1.0
    entries = jax.random.normal(stream_key, shape, jnp.float32) * deviation * gain
    return jnp.minimum(jnp.maximum(entries, -most), most).astype(dtype)


def setup_inputs(seed: int = 0) -> dict:
    seeds = jax.random.split(jax.random.key(seed), 16)
    hidden_in = centred(seeds[0], (TOKENS, D), 1.0, 6.0, ((0, 8), (1, 4)))
    norm_gain = jnp.clip(1.0 + 0.1 * jax.random.normal(seeds[1], (D,), jnp.float32), 0.5, 1.5)
    w_x = centred(seeds[2], (D, DI), D ** -0.5, 0.09375, ((0, 8), (1, 4)))
    w_z = centred(seeds[3], (D, DI), D ** -0.5, 0.09375, ((0, 8), (1, 4)))
    w_bc = centred(seeds[4], (D, G, 2 * N), D ** -0.5, 0.09375, ((0, 8), (1, 4)))
    w_dt = centred(seeds[5], (D, H), D ** -0.5, 0.09375, ((0, 8), (1, 4)))
    dt_bias = jnp.clip(-6.0 + 4.0 * jax.random.uniform(seeds[6], (H,), jnp.float32) ** shard_levels(seeds[6], (H,), ((0, 4),), -0.2, 0.2), -6.0, -2.0)
    decay_rate = jnp.clip(jnp.exp(math.log(8.0) - 10.109526 * jax.random.uniform(seeds[7], (H,), jnp.float32) ** shard_levels(seeds[7], (H,), ((0, 4),), -0.2, 0.2)), 0.00032552084, 8.0)
    conv_x = centred(seeds[8], (KCONV, DI), KCONV ** -0.5, 3.0, ((1, 4),), jnp.float32)
    conv_bc = centred(seeds[9], (KCONV, G, 2 * N), KCONV ** -0.5, 3.0, ((1, 4),), jnp.float32)
    conv_bias_x = centred(seeds[10], (DI,), 0.5, 3.0, ((0, 4),), jnp.float32)
    conv_bias_bc = centred(seeds[11], (G, 2 * N), 0.5, 3.0, ((0, 4),), jnp.float32)
    skip_d = jnp.clip(jnp.exp(math.log(8.0) - 2.7725887 * jax.random.uniform(seeds[12], (H,), jnp.float32) ** shard_levels(seeds[12], (H,), ((0, 4),), -0.2, 0.2)), 0.5, 8.0)
    out_gain = jnp.clip(1.0 + 0.1 * jax.random.normal(seeds[13], (DI,), jnp.float32), 0.5, 1.5)
    w_out = centred(seeds[14], (DI, D), DI ** -0.5, 0.0625, ((0, 4),))
    return {"hidden_in": hidden_in, "norm_gain": norm_gain, "w_x": w_x, "w_z": w_z, "w_bc": w_bc, "w_dt": w_dt, "dt_bias": dt_bias, "decay_rate": decay_rate, "conv_x": conv_x, "conv_bc": conv_bc, "conv_bias_x": conv_bias_x, "conv_bias_bc": conv_bias_bc, "skip_d": skip_d, "out_gain": out_gain, "w_out": w_out}


epsilon = 1e-05

def rms_scale(values, norm_weight):
    return values * lax.rsqrt(lax.optimization_barrier(jnp.mean(values * values, axis=-1, keepdims=True)) + epsilon) * norm_weight

def causal_conv(padded, weight, bias_row):
    tap_count = weight.shape[0]
    out_length = padded.shape[0] - tap_count + 1
    running = bias_row.astype(jnp.float32)
    for k in range(tap_count):
        running = running + weight[k].astype(jnp.float32) * padded[k:k + out_length].astype(jnp.float32)
    return jax.nn.silu(running).astype(jnp.bfloat16)

def span_terms(x_blocks, b_blocks, c_blocks, log_decay, dt_blocks):
    cum_decay = jnp.cumsum(log_decay, axis=1)
    scores = jnp.einsum('ctgn,csgn->cgts', c_blocks.astype(jnp.float32), b_blocks.astype(jnp.float32))
    length = x_blocks.shape[1]
    causal_mask = lax.broadcasted_iota(jnp.int32, (length, length), 0) >= lax.broadcasted_iota(jnp.int32, (length, length), 1)
    cum_rows = jnp.transpose(cum_decay, (0, 2, 3, 1))
    decay_gap = cum_rows[..., :, None] - cum_rows[..., None, :]
    decay_mat = jnp.where(causal_mask, jnp.exp(jnp.where(causal_mask, decay_gap, 0.0)), 0.0)
    dt_cols = jnp.transpose(dt_blocks, (0, 2, 3, 1))[..., None, :]
    mix_weight = (scores[:, :, None] * decay_mat * dt_cols).astype(jnp.bfloat16)
    intra_out = jnp.einsum('cgkts,csgkp->ctgkp', mix_weight.astype(jnp.float32), x_blocks.astype(jnp.float32))
    tail_decay = jnp.exp(cum_decay[:, -1:] - cum_decay) * dt_blocks
    scaled = (x_blocks.astype(jnp.float32) * tail_decay[..., None]).astype(jnp.bfloat16)
    fresh_state = jnp.einsum('csgkp,csgn->cgkpn', scaled.astype(jnp.float32), b_blocks.astype(jnp.float32))
    return (cum_decay, intra_out, fresh_state)

def reference(hidden_in, norm_gain, w_x, w_z, w_bc, w_dt, dt_bias, decay_rate, conv_x, conv_bc, conv_bias_x, conv_bias_bc, skip_d, out_gain, w_out):
    per_group = H // G
    span_count = TOKENS // SPAN
    rim_rows = KCONV - 1
    normed = rms_scale(hidden_in.astype(jnp.float32), norm_gain).astype(jnp.bfloat16)
    proj_x = jnp.dot(normed, w_x, preferred_element_type=jnp.float32).astype(jnp.bfloat16)
    gate_z = jnp.dot(normed, w_z, preferred_element_type=jnp.float32).astype(jnp.bfloat16)
    proj_bc = jnp.dot(normed, w_bc.reshape(D, G * 2 * N), preferred_element_type=jnp.float32).astype(jnp.bfloat16).reshape(TOKENS, G, 2 * N)
    dt_vals = jax.nn.softplus(jnp.dot(normed, w_dt, preferred_element_type=jnp.float32) + dt_bias)
    x_conv = causal_conv(jnp.concatenate([jnp.zeros((rim_rows, DI), jnp.bfloat16), proj_x], axis=0), conv_x, conv_bias_x)
    bc_conv = causal_conv(jnp.concatenate([jnp.zeros((rim_rows, G, 2 * N), jnp.bfloat16), proj_bc], axis=0), conv_bc, conv_bias_bc)
    x_blocks = x_conv.reshape(span_count, SPAN, G, per_group, P_SIZE)
    b_blocks = bc_conv[..., :N].reshape(span_count, SPAN, G, N)
    c_blocks = bc_conv[..., N:].reshape(span_count, SPAN, G, N)
    log_decay = (-dt_vals * decay_rate).reshape(span_count, SPAN, G, per_group)
    dt_blocks = dt_vals.reshape(span_count, SPAN, G, per_group)
    skip_heads = skip_d.reshape(G, per_group)[..., None]

    def span_step(state_in, block_item):
        x_block, b_block, c_block, log_block, dt_block = [piece[None] for piece in block_item]
        cum_decay, intra_out, fresh_state = span_terms(x_block, b_block, c_block, log_block, dt_block)
        inter_out = jnp.exp(cum_decay)[..., None] * jnp.einsum('ctgn,gkpn->ctgkp', c_block.astype(jnp.float32), state_in, precision=lax.Precision.HIGHEST)
        ssm_out = intra_out + inter_out + skip_heads * x_block.astype(jnp.float32)
        state_next = jnp.exp(cum_decay[0, -1])[..., None, None] * state_in + fresh_state[0]
        return (state_next, ssm_out[0])
    start_state = jnp.zeros((G, per_group, P_SIZE, N), jnp.float32)
    final_state, ssm_out = lax.scan(span_step, start_state, (x_blocks, b_blocks, c_blocks, log_decay, dt_blocks))
    ssm_out = ssm_out.reshape(TOKENS, DI)
    gated_out = ssm_out * jax.nn.silu(gate_z.astype(jnp.float32))
    grouped = gated_out.reshape(TOKENS, G, DI // G)
    normed_y = rms_scale(grouped, out_gain.reshape(G, DI // G)).reshape(TOKENS, DI).astype(jnp.bfloat16)
    mixed = jnp.dot(normed_y, w_out, preferred_element_type=jnp.float32)
    return (hidden_in.astype(jnp.float32) + mixed).astype(jnp.bfloat16)
```

```python
import jax
import jax.numpy as jnp
from jax import lax
from jax.sharding import Mesh, PartitionSpec as P

SPAN = 128
RING_LIMIT = 8


epsilon = 1e-05


def rms_scale(values, norm_weight):
    return (
        values
        * lax.rsqrt(jnp.mean(values * values, axis=-1, keepdims=True) + epsilon)
        * norm_weight
    )


def causal_conv(padded, weight, bias_row):
    tap_count = weight.shape[0]
    out_length = padded.shape[0] - tap_count + 1
    running = bias_row
    for k in range(tap_count):
        running = running + weight[k] * padded[k : k + out_length].astype(jnp.float32)
    return jax.nn.silu(running).astype(jnp.bfloat16)


def span_terms(x_blocks, b_blocks, c_blocks, log_decay, dt_blocks):
    cum_decay = jnp.cumsum(log_decay, axis=1)
    scores = jnp.einsum("ctgn,csgn->cgts", c_blocks, b_blocks, preferred_element_type=jnp.float32)
    length = x_blocks.shape[1]
    causal_mask = lax.broadcasted_iota(jnp.int32, (length, length), 0) >= lax.broadcasted_iota(
        jnp.int32, (length, length), 1
    )
    cum_rows = jnp.transpose(cum_decay, (0, 2, 3, 1))
    decay_gap = cum_rows[..., :, None] - cum_rows[..., None, :]
    decay_mat = jnp.where(causal_mask, jnp.exp(jnp.where(causal_mask, decay_gap, 0.0)), 0.0)
    dt_cols = jnp.transpose(dt_blocks, (0, 2, 3, 1))[..., None, :]
    mix_weight = (scores[:, :, None] * decay_mat * dt_cols).astype(jnp.bfloat16)
    intra_out = jnp.einsum(
        "cgkts,csgkp->ctgkp", mix_weight, x_blocks, preferred_element_type=jnp.float32
    )
    tail_decay = jnp.exp(cum_decay[:, -1:] - cum_decay) * dt_blocks
    scaled = (x_blocks.astype(jnp.float32) * tail_decay[..., None]).astype(jnp.bfloat16)
    fresh_state = jnp.einsum(
        "csgkp,csgn->cgkpn", scaled, b_blocks, preferred_element_type=jnp.float32
    )
    return (cum_decay, intra_out, fresh_state)


def shifted(block, axis, distance):
    count = lax.axis_size(axis)
    return lax.ppermute(block, axis, [(i, (i + distance) % count) for i in range(count)])


def passed_along(block, axis, distance):
    devices = range(lax.axis_size(axis))
    return lax.ppermute(block, axis, [(i - distance, i) for i in devices if i - distance in devices])


def swapped(block, axis, bit):
    return lax.ppermute(block, axis, [(i, i ^ bit) for i in range(lax.axis_size(axis))])


def ring_pieces(own, axis):
    count = lax.axis_size(axis)
    pieces = [(0, 0, own)]
    ahead, behind = own, own
    for step in range(1, (count - 1) // 2 + 1):
        ahead, behind = shifted(ahead, axis, 1), shifted(behind, axis, -1)
        pieces += [(step, 0, ahead), (count - step, 0, behind)]
    if count % 2 == 0:
        half = own.shape[0] // 2
        pieces += [
            (count // 2, 0, shifted(ahead[:half], axis, 1)),
            (count // 2, half, shifted(behind[half:], axis, -1)),
        ]
    return pieces


def carried_in(total_log, state):
    count, mine = lax.axis_size("outer"), lax.axis_index("outer")
    logs, states = lax.all_gather((total_log, state), "outer")

    def hop(position, running):
        longer = jnp.exp(logs[position])[..., None, None] * running + states[position]
        return jnp.where(position < mine, longer, running)

    return lax.fori_loop(0, count - 1, hop, jnp.zeros_like(state))


def gather_tokens(hidden_in):
    tensor, fold = lax.axis_size("tensor"), lax.axis_size("fold")
    rows, cols = hidden_in.shape
    pieces = [(0, 0, hidden_in)]
    bits = []
    bit = tensor // 2
    while bit > 1:
        bits.append(("tensor", bit))
        bit //= 2
    if fold > 1:
        bits.append(("fold", 1))
    if tensor > 1:
        bits.append(("tensor", 1))
    for axis, bit in bits:
        pieces += [
            (j ^ bit, k, swapped(part, axis, bit)) if axis == "tensor" else (j, k ^ bit, swapped(part, axis, bit))
            for j, k, part in list(pieces)
        ]
    full = jnp.zeros((tensor, rows * fold, cols), hidden_in.dtype)
    me_t, me_f = lax.axis_index("tensor"), lax.axis_index("fold")
    for j, k, part in pieces:
        full = lax.dynamic_update_slice(full, part[None], (me_t ^ j, (me_f ^ k) * rows, 0))
    return full


def scatter_sum(partial, rows, cols):
    tensor, fold = lax.axis_size("tensor"), lax.axis_size("fold")
    me_t, me_f = lax.axis_index("tensor"), lax.axis_index("fold")
    if tensor > 1:
        pairs = partial.reshape(fold * rows, tensor // 2, 2, cols)
        core = me_t % 2
        keep = lax.dynamic_index_in_dim(pairs, core, 2, keepdims=False)
        send = lax.dynamic_index_in_dim(pairs, 1 - core, 2, keepdims=False)
        keep = keep.astype(jnp.float32) + swapped(send.astype(jnp.bfloat16), "tensor", 1).astype(jnp.float32)
    else:
        keep = partial.reshape(fold * rows, 1, cols).astype(jnp.float32)

    def over_fold(value):
        if fold == 1:
            return value
        split = value.reshape(fold, rows, *value.shape[1:])
        mine = lax.dynamic_index_in_dim(split, me_f, 0, keepdims=False)
        other = lax.dynamic_index_in_dim(split, 1 - me_f, 0, keepdims=False)
        return mine + swapped(other.astype(jnp.bfloat16), "fold", 1).astype(jnp.float32)

    def over_high(value):
        count = tensor // 2
        bit = tensor // 2
        while count > 1:
            split = value.reshape(value.shape[0], 2, count // 2, value.shape[-1])
            top = (me_t // bit) % 2
            mine = lax.dynamic_index_in_dim(split, top, 1, keepdims=False)
            other = lax.dynamic_index_in_dim(split, 1 - top, 1, keepdims=False)
            value = mine + swapped(other.astype(jnp.bfloat16), "tensor", bit).astype(jnp.float32)
            count, bit = count // 2, bit // 2
        return value

    half = cols // 2
    first = over_high(over_fold(keep[..., :half]))
    second = over_fold(over_high(keep[..., half:]))
    return jnp.concatenate([first.reshape(rows, half), second.reshape(rows, cols - half)], axis=1)


def local(
    hidden_in,
    norm_gain,
    w_x,
    w_z,
    w_bc,
    w_dt,
    dt_bias,
    decay_rate,
    conv_x,
    conv_bc,
    conv_bias_x,
    conv_bias_bc,
    skip_d,
    out_gain,
    w_out,
):
    fold = lax.axis_size("fold")
    me_f = lax.axis_index("fold")
    me_o = lax.axis_index("outer")
    outer = lax.axis_size("outer")

    def part(value, axis, which=None):
        size = value.shape[axis] // fold
        which = me_f if which is None else which
        return lax.dynamic_slice_in_dim(value, which * size, size, axis)

    depth = w_x.shape[0]
    groups = w_bc.shape[1] // fold
    bc_width = w_bc.shape[2]
    bc_flat = w_bc.reshape(depth, w_bc.shape[1] * bc_width)
    state_dim = bc_width // 2
    head_count = decay_rate.shape[0] // fold
    inner_width = w_x.shape[1] // fold
    head_dim = inner_width // head_count
    per_group = head_count // groups

    def weights(which):
        side = jnp.concatenate([part(bc_flat, 1, which), part(w_dt, 1, which)], axis=1)
        return [jnp.concatenate([part(w_x, 1, which), side], axis=1), part(w_z, 1, which)]

    own = weights(me_f)
    other = [swapped(block, "fold", 1) for block in weights(1 - me_f)] if fold > 1 else []
    gathered = gather_tokens(hidden_in)
    blocks, row_count, width = gathered.shape
    values = gathered.astype(jnp.float32)
    scale = lax.rsqrt(jnp.mean(values * values, axis=(0, 2), keepdims=True) + epsilon)
    normed = (values * scale * norm_gain.reshape(blocks, 1, width)).astype(jnp.bfloat16)
    per_block = max(width // depth, 1)
    if outer <= RING_LIMIT:
        normed = normed.reshape(blocks, row_count, per_block, width // per_block)
        normed = jnp.transpose(normed, (0, 2, 1, 3)).reshape(blocks * per_block, row_count, depth)
    else:
        normed = jnp.transpose(normed, (1, 0, 2)).reshape(row_count, blocks * width)
    rim_rows = conv_x.shape[0] - 1

    def projected(index):
        total = None
        if outer > RING_LIMIT:
            rows = lax.all_gather(own[index], "outer")
            if fold > 1:
                theirs = lax.all_gather(other[index], "outer")
                first, second = jnp.where(me_f == 0, rows, theirs), jnp.where(me_f == 0, theirs, rows)
                rows = jnp.stack([first, second], axis=1)
            rows = rows.reshape(normed.shape[1], own[index].shape[1])
            return jnp.dot(normed, rows, preferred_element_type=jnp.float32)
        for k, block in enumerate([own, other] if fold > 1 else [own]):
            for behind, offset, piece in ring_pieces(block[index], "outer"):
                owner = (me_o - behind + outer) % outer
                lhs = lax.dynamic_index_in_dim(normed, owner * fold + (me_f ^ k), 0, keepdims=False)
                lhs = lhs[:, offset : offset + piece.shape[0]]
                term = jnp.dot(lhs, piece, preferred_element_type=jnp.float32)
                total = term if total is None else total + term
        return total

    first = projected(0)
    proj_x = first[:, :inner_width].astype(jnp.bfloat16)
    side = first[:, inner_width:]
    dt_raw = side[:, groups * bc_width :]
    proj_bc = side[:, : groups * bc_width].astype(jnp.bfloat16)
    gate_z = projected(1).astype(jnp.bfloat16)
    edge_x, edge_bc = passed_along(
        (proj_x[row_count - rim_rows :], proj_bc[row_count - rim_rows :]), "outer", 1
    )
    padded_x = jnp.concatenate([edge_x, proj_x], axis=0)
    padded_bc = jnp.concatenate([edge_bc, proj_bc], axis=0)
    dt_vals = jax.nn.softplus(dt_raw + part(dt_bias, 0))
    x_conv = causal_conv(padded_x, part(conv_x, 1), part(conv_bias_x, 0))
    bc_conv = causal_conv(
        padded_bc,
        part(conv_bc, 1).reshape(conv_bc.shape[0], groups * bc_width),
        part(conv_bias_bc, 0).reshape(groups * bc_width),
    ).reshape(row_count, groups, bc_width)
    span_count = row_count // SPAN
    x_blocks = x_conv.reshape(span_count, SPAN, groups, per_group, head_dim)
    b_blocks = bc_conv[..., :state_dim].reshape(span_count, SPAN, groups, state_dim)
    c_blocks = bc_conv[..., state_dim:].reshape(span_count, SPAN, groups, state_dim)
    log_decay = (-dt_vals * part(decay_rate, 0)).reshape(span_count, SPAN, groups, per_group)
    dt_blocks = dt_vals.reshape(span_count, SPAN, groups, per_group)
    cum_decay, intra_out, fresh_state = span_terms(
        x_blocks, b_blocks, c_blocks, log_decay, dt_blocks
    )
    block_totals = cum_decay[:, -1]
    state = jnp.zeros((groups, per_group, head_dim, state_dim), jnp.float32)
    entering = []
    for i in range(span_count):
        entering.append(state)
        state = jnp.exp(block_totals[i])[..., None, None] * state + fresh_state[i]
    local_enter = jnp.stack(entering)
    before_log = jnp.cumsum(block_totals, axis=0) - block_totals
    total_log = jnp.sum(block_totals, axis=0)
    if outer > RING_LIMIT:
        incoming = carried_in(total_log, state)
    else:
        incoming = jnp.zeros_like(state)
        log_between = jnp.zeros_like(total_log)
        for distance in range(1, outer):
            arrived = passed_along(state, "outer", distance)
            incoming = incoming + jnp.exp(log_between)[..., None, None] * arrived
            log_between = log_between + passed_along(total_log, "outer", distance)
    enter_state = local_enter + jnp.exp(before_log)[..., None, None] * incoming[None]
    inter_out = jnp.exp(cum_decay)[..., None] * jnp.einsum(
        "ctgn,cgkpn->ctgkp", c_blocks, enter_state.astype(jnp.bfloat16), preferred_element_type=jnp.float32
    )
    skip_heads = part(skip_d, 0).reshape(groups, per_group)[..., None]
    ssm_out = (intra_out + inter_out + skip_heads * x_blocks.astype(jnp.float32)).reshape(
        row_count, inner_width
    )
    gated_out = ssm_out * jax.nn.silu(gate_z.astype(jnp.float32))
    grouped = gated_out.reshape(row_count, groups, inner_width // groups)
    normed_y = (
        rms_scale(grouped, part(out_gain, 0).reshape(groups, inner_width // groups))
        .reshape(row_count, inner_width)
        .astype(jnp.bfloat16)
    )
    partial = jnp.dot(normed_y, part(w_out, 0), preferred_element_type=jnp.float32)
    summed = scatter_sum(partial, *hidden_in.shape)
    return (hidden_in.astype(jnp.float32) + summed).astype(jnp.bfloat16)


def solution(mesh):
    seq, tensor = mesh.shape["seq"], mesh.shape["tensor"]

    def run(*args):
        groups = args[4].shape[1] // tensor
        fold = 2 if groups % 2 == 0 and seq % 2 == 0 else 1
        split = Mesh(
            mesh.devices.reshape(seq // fold, fold, tensor), ("outer", "fold", "tensor")
        )
        both = ("outer", "fold")
        in_specs = (
            P(both, "tensor"),
            P(),
            P(both, "tensor"),
            P(both, "tensor"),
            P(both, "tensor", None),
            P(both, "tensor"),
            P("tensor"),
            P("tensor"),
            P(None, "tensor"),
            P(None, "tensor", None),
            P("tensor"),
            P("tensor", None),
            P("tensor"),
            P("tensor"),
            P("tensor", None),
        )
        return jax.shard_map(
            local, mesh=split, in_specs=in_specs, out_specs=P(both, "tensor"), check_vma=False
        )(*args)

    return run
```
